32 devices in a mesh: section: 2 (over x), dp: 16 (over z, y, core).
Axes of the slice: x: 2, y: 2, z: 4, core: 2. Of those that a mesh axis runs over, the one named last changes fastest.
Arguments:
- activations: bfloat16 [2, 8, 768, 5376], P('section', None, 'dp'), may hold values from -6 to 6
- loss_grads: bfloat16 [8, 768, 5376], P(None, 'dp'), may hold values from -6 to 6
- adapter_in: bfloat16 [2, 5376, 64], P('section'), may hold values from -0.078125 to 0.078125
- adapter_out: bfloat16 [2, 64, 5376], P('section'), may hold values from -0.75 to 0.75
- first_moment: float32 [2, 16, 86016], P('section', 'dp'), may hold values from -0.4 to 0.4
- second_moment: float32 [2, 16, 86016], P('section', 'dp'), may hold values from 0.0001 to 0.01
- old_owner: int32 [2, 8], P('section'), may hold values from 0 to 15, as said below
- new_owner: int32 [2, 16], P('section'), may hold values from 0 to 15, each once within a row
- plan: int32 [8], replicated, may hold values from 0 to 7, each once
Outputs:
- input_grads: bfloat16 [2, 8, 768, 5376], P('section', None, 'dp')
- adam_update: float32 [2, 16, 43008], P('section', 'dp')
- first_new: float32 [2, 16, 43008], P('section', 'dp')
- second_new: float32 [2, 16, 43008], P('section', 'dp')
The draws below stay inside these ranges and needn't reach their ends.
Inputs may be any that keep to these rules, and one draw needn't show every extreme that they name: `old_owner`: the entries of one section's row are distinct.
All inputs are finite; a program needn't handle non-finite values.
Results may differ from the reference program's by a relative error of at most 0.025.
Values may be sent and summed in bfloat16 or wider, within the bound.
A program may use at most 64 MiB of HBM per device.

```python
import math
import jax
import jax.numpy as jnp

D = 5376
RANK = 64
MB = 8
SECTIONS = 2
TOKENS = 768
BLOCK = 43008
OLD_DP = 8
N_DP = 16


def draw_old_owner(key, part):
    section_keys = jax.random.split(key, SECTIONS)
    rows = jax.vmap(lambda section_key: jax.random.permutation(section_key, N_DP)[:OLD_DP])(section_keys)
    return rows.astype(jnp.int32)


def strengthened(drawn, key, source, target, parts, factor):
    owner, partner = [(jnp.arange(drawn.shape[axis_at]) // (drawn.shape[axis_at] // parts)).reshape([-1 if axis == axis_at else 1 for axis in range(drawn.ndim)]) for axis_at in (source, target)]
    chosen = jax.random.permutation(key, parts)[partner]
    strong = (owner == chosen) | (owner == (partner + parts // 2) % parts)
    return jnp.where(strong, factor * drawn, drawn)


def levels(key, shape, cuts, low, largest):
    loudness, own = 1.0, jax.random.fold_in(key, 6)
    for dim, blocks in cuts:
        steps = jnp.exp(jax.random.uniform(jax.random.fold_in(own, dim), (blocks,), jnp.float32, low / len(cuts), largest / len(cuts)))
        loudness = loudness * jnp.repeat(steps, shape[dim] // blocks).reshape([-1 if axis == dim else 1 for axis in range(len(shape))])
    return loudness


def bell_draw(stream_key, shape, width, bound, cuts=(), kind=jnp.bfloat16):
    array = jax.random.normal(stream_key, shape, jnp.float32) * width
    if len(cuts) > 0:
        array = levels(stream_key, shape, cuts, -0.22, 0.18) * array
    return jnp.clip(array, min=-bound, max=bound).astype(kind)


def heavy_noise(rng, dims, width, reach, shards, heavy, kind=jnp.bfloat16):
    array = width * jax.random.normal(rng, dims, jnp.float32)
    if shards:
        array = array * levels(rng, dims, shards, -0.22, 0.18)
    return jnp.clip(strengthened(array, jax.random.fold_in(rng, 3), *heavy), -reach, reach).astype(kind)


def setup_inputs(seed: int = 0) -> dict:
    key_of = jax.random.split(jax.random.key(seed), 10)
    activations = bell_draw(key_of[0], (SECTIONS, MB, TOKENS, D), 1.0, 6.0, ((0, 2), (2, 16)))
    loss_grads = heavy_noise(key_of[1], (MB, TOKENS, D), 1.0, 6.0, ((1, 16),), (1, 2, 16, 2.0))
    adapter_in = bell_draw(key_of[2], (SECTIONS, D, RANK), D ** -0.5, 0.078125, ((0, 2),))
    adapter_out = bell_draw(key_of[3], (SECTIONS, RANK, D), RANK ** -0.5, 0.75, ((0, 2),))
    first_moment = bell_draw(key_of[4], (SECTIONS, N_DP, 2 * BLOCK), 0.05, 0.4, ((0, 2), (1, 16)), jnp.float32)
    second_moment = jnp.clip(jnp.exp(math.log(0.01) - 4.6051702 * jax.random.uniform(key_of[5], (SECTIONS, N_DP, 2 * BLOCK), jnp.float32) ** levels(key_of[5], (SECTIONS, N_DP, 2 * BLOCK), ((0, 2), (1, 16)), -0.2, 0.2)), 0.0001, 0.01)
    old_owner = draw_old_owner(jax.random.fold_in(key_of[9], 71), 0)
    new_owner = jax.vmap(lambda own: jax.random.permutation(own, N_DP))(jax.random.split(key_of[7], SECTIONS)).reshape((SECTIONS, N_DP)).astype(jnp.int32)
    plan = jax.random.permutation(key_of[8], MB).astype(jnp.int32)
    return dict(activations=activations, loss_grads=loss_grads, adapter_in=adapter_in, adapter_out=adapter_out, first_moment=first_moment, second_moment=second_moment, old_owner=old_owner, new_owner=new_owner, plan=plan)


beta_one = 0.9
beta_two = 0.95
adam_eps = 1e-08
adam_step = 1000.0
loss_scale = 4096.0

def silu_slope(pre_value):
    gate_value = jax.nn.sigmoid(pre_value)
    return gate_value * (1.0 + pre_value * (1.0 - gate_value))

def adam_rows(grads, first, second):
    first_next = beta_one * first + (1.0 - beta_one) * grads
    second_next = beta_two * second + (1.0 - beta_two) * grads * grads
    update = first_next / (1.0 - beta_one ** adam_step) / (jnp.sqrt(second_next / (1.0 - beta_two ** adam_step)) + adam_eps)
    return (update, first_next, second_next)

def reference(activations, loss_grads, adapter_in, adapter_out, first_moment, second_moment, old_owner, new_owner, plan):
    incoming = loss_grads[plan]
    emitted = []
    updates = []
    firsts = []
    seconds = []
    for section_index in reversed(range(SECTIONS)):
        section_input = activations[section_index][plan].reshape(-1, D)
        incoming_flat = incoming.reshape(-1, D)
        weight_in = adapter_in[section_index]
        weight_out = adapter_out[section_index]
        pre_value = jnp.dot(section_input, weight_in, preferred_element_type=jnp.float32)
        hidden = jax.nn.silu(pre_value).astype(jnp.bfloat16)
        act_grad = jnp.dot(incoming_flat, weight_out.T, preferred_element_type=jnp.float32)
        pre_grad = (act_grad * silu_slope(pre_value)).astype(jnp.bfloat16)
        input_grad = (incoming_flat.astype(jnp.float32) + jnp.dot(pre_grad, weight_in.T, preferred_element_type=jnp.float32)).astype(jnp.bfloat16)
        grad_in = jnp.dot(section_input.T, pre_grad, preferred_element_type=jnp.float32)
        grad_out = jnp.dot(hidden.T, incoming_flat, preferred_element_type=jnp.float32)
        grads = jnp.concatenate([grad_in.reshape(-1), grad_out.reshape(-1)]) / loss_scale
        first_old = first_moment[section_index][old_owner[section_index]].reshape(-1)
        second_old = second_moment[section_index][old_owner[section_index]].reshape(-1)
        update, first_next, second_next = adam_rows(grads, first_old, second_old)
        inverse = jnp.argsort(new_owner[section_index]).astype(jnp.int32)
        updates.insert(0, update.reshape(N_DP, BLOCK)[inverse])
        firsts.insert(0, first_next.reshape(N_DP, BLOCK)[inverse])
        seconds.insert(0, second_next.reshape(N_DP, BLOCK)[inverse])
        incoming = input_grad.reshape(MB, TOKENS, D)
        emitted.insert(0, incoming)
    return (jnp.stack(emitted), jnp.stack(updates), jnp.stack(firsts), jnp.stack(seconds))
```

```python
import functools
import math

import jax
import jax.numpy as jnp
from jax import lax
from jax.experimental import pallas as pl
from jax.experimental.pallas import tpu as pltpu
from jax.sharding import PartitionSpec as P

beta_one = 0.9
beta_two = 0.95
adam_eps = 1e-08
adam_step = 1000.0
loss_scale = 4096.0
MESH = pl.DeviceIdType.MESH
VMEM = pl.BlockSpec(memory_space=pltpu.VMEM)
SMEM = pl.BlockSpec(memory_space=pltpu.SMEM)
ANY = pl.BlockSpec(memory_space=pl.ANY)


def nt_dot(left, right):
    return lax.dot_general(left, right, (((1,), (1,)), ((), ())), preferred_element_type=jnp.float32)


def column_width(width):
    return 128 * max(d for d in range(1, 8) if (width // 128) % d == 0)


def greet(n, me, extra):
    barrier = pltpu.get_barrier_semaphore()

    @pl.loop(1, n)
    def _(d):
        pl.semaphore_signal(barrier, inc=1, device_id={"dp": lax.rem(me + d, n)}, device_id_type=MESH)

    if extra is not None:
        pl.semaphore_signal(barrier, inc=1, device_id={"section": extra}, device_id_type=MESH)
    pl.semaphore_wait(barrier, n - 1 + (extra is not None))


def exchange_kernel(
    n, x_hbm, l_hbm, win_ref, wout_ref, pieces_ref, pick_ref,
    pre_ref, p_ref, w_ref, got_ref,
    x_buf, l_buf, p_buf, spread, chosen,
    x_sem, l_sem, w_send, w_recv, f_send, f_recv, p_send, p_recv, a_send, a_recv, b_send, b_recv, own_sem,
):
    me = lax.axis_index("dp")
    other = 1 - lax.axis_index("section")
    core = lax.rem(me, 2)
    sibling = me + 1 - 2 * core
    rank, width = win_ref.shape
    cw = column_width(width)
    chunks = width // cw
    loads = []
    for c in range(chunks):
        cols = pl.ds(c * cw, cw)
        for src, dst, sem in ((x_hbm, x_buf, x_sem), (l_hbm, l_buf, l_sem)):
            load = pltpu.make_async_copy(src.at[:, cols], dst.at[:, cols], sem.at[c])
            load.start()
            loads.append(load)
    own = pltpu.make_async_copy(pieces_ref.at[me], spread.at[me], own_sem.at[0])
    own.start()
    greet(n, me, other)
    half = rank // 2
    mine = pl.ds(pl.multiple_of(core * half, half), half)
    theirs = pl.ds(pl.multiple_of((1 - core) * half, half), half)
    w_copy = pltpu.make_async_remote_copy(
        win_ref.at[mine], w_ref.at[mine], w_send, w_recv, device_id={"section": other}, device_id_type=MESH
    )
    w_copy.start()

    def spread_copy(d):
        peer = lax.rem(me + d, n)
        return pltpu.make_async_remote_copy(
            pieces_ref.at[peer], spread.at[me], a_send.at[d], a_recv.at[d],
            device_id={"dp": peer}, device_id_type=MESH,
        )

    def spread_arrival(d):
        peer = lax.rem(me + n - d, n)
        return pltpu.make_async_remote_copy(
            pieces_ref.at[peer], spread.at[peer], a_send.at[d], a_recv.at[d],
            device_id={"dp": peer}, device_id_type=MESH,
        )

    def gather_copy(d):
        peer = lax.rem(me + d, n)
        return pltpu.make_async_remote_copy(
            chosen.at[peer], got_ref.at[me], b_send.at[d], b_recv.at[d],
            device_id={"dp": peer}, device_id_type=MESH,
        )

    def gather_arrival(d):
        peer = lax.rem(me + n - d, n)
        return pltpu.make_async_remote_copy(
            chosen.at[peer], got_ref.at[peer], b_send.at[d], b_recv.at[d],
            device_id={"dp": peer}, device_id_type=MESH,
        )

    @pl.loop(1, n)
    def _(d):
        spread_copy(d).start()

    rows = x_buf.shape[0]
    pre = jnp.zeros((rows, rank), jnp.float32)
    act = jnp.zeros((rows, rank), jnp.float32)
    for c in range(chunks):
        cols = pl.ds(c * cw, cw)
        loads[2 * c].wait()
        loads[2 * c + 1].wait()
        pre = pre + nt_dot(x_buf[:, cols], win_ref[:, cols])
        act = act + nt_dot(l_buf[:, cols], wout_ref[:, cols])
    pre_ref[...] = pre
    p_buf[...] = (act * silu_slope(pre)).astype(jnp.bfloat16)
    p_copy = pltpu.make_async_remote_copy(
        p_buf, p_ref, p_send, p_recv, device_id={"section": other}, device_id_type=MESH
    )
    p_copy.start()
    own.wait()

    @pl.loop(1, n)
    def _(d):
        spread_arrival(d).wait_recv()

    for t in range(n):
        chosen[t] = spread[pick_ref[t, 0], pick_ref[t, 1]]

    @pl.loop(1, n)
    def _(d):
        gather_copy(d).start()

    keep = pltpu.make_async_copy(chosen.at[me], got_ref.at[me], own_sem.at[1])
    keep.start()
    w_copy.wait_recv()
    forward = pltpu.make_async_remote_copy(
        w_ref.at[mine], w_ref.at[mine], f_send, f_recv, device_id={"dp": sibling}, device_id_type=MESH
    )
    forward.start()
    w_copy.wait_send()
    p_copy.wait()
    forward.wait_send()
    pltpu.make_async_remote_copy(
        w_ref.at[theirs], w_ref.at[theirs], f_send, f_recv, device_id={"dp": sibling}, device_id_type=MESH
    ).wait_recv()
    keep.wait()

    @pl.loop(1, n)
    def _(d):
        spread_copy(d).wait_send()
        gather_copy(d).wait_send()
        gather_arrival(d).wait_recv()


def exchange(n, x, loss, win, wout, pieces, picks):
    rows, width = x.shape
    rank = win.shape[0]
    chunks = width // column_width(width)
    dma = pltpu.SemaphoreType.DMA
    return pl.pallas_call(
        functools.partial(exchange_kernel, n),
        out_shape=(
            jax.ShapeDtypeStruct((rows, rank), jnp.float32),
            jax.ShapeDtypeStruct((rows, rank), jnp.bfloat16),
            jax.ShapeDtypeStruct((rank, width), jnp.bfloat16),
            jax.ShapeDtypeStruct((n,) + pieces.shape[2:], jnp.bfloat16),
        ),
        in_specs=[ANY, ANY, VMEM, VMEM, VMEM, SMEM],
        out_specs=(VMEM,) * 4,
        scratch_shapes=[
            pltpu.VMEM(x.shape, jnp.bfloat16),
            pltpu.VMEM(x.shape, jnp.bfloat16),
            pltpu.VMEM((rows, rank), jnp.bfloat16),
            pltpu.VMEM(pieces.shape, jnp.bfloat16),
            pltpu.VMEM((n,) + pieces.shape[2:], jnp.bfloat16),
            dma((chunks,)), dma((chunks,)), dma, dma, dma, dma, dma, dma,
            dma((n,)), dma((n,)), dma((n,)), dma((n,)), dma((2,)),
        ],
        compiler_params=pltpu.CompilerParams(collective_id=0, has_side_effects=True),
        name="exchange",
    )(x, loss, win, wout, pieces, picks)


def drain_kernel(
    n, relayed_ref, slot_ref, place_ref, x_hbm, l_hbm, pre_ref, p_in_ref, w_up_ref, win_ref, wout_ref,
    out_hbm, q_ref,
    x_buf, l_buf, o_buf, gin, gout, turn, x_sem, l_sem, o_sem,
):
    rank, width = win_ref.shape
    micro_count, tok_rows, _ = out_hbm.shape
    cw = column_width(width)
    chunks = width // cw
    loads_x, loads_l = [], []
    for c in range(chunks):
        cols = pl.ds(c * cw, cw)
        loads_l.append(pltpu.make_async_copy(l_hbm.at[:, cols], l_buf.at[:, cols], l_sem.at[c]))
        loads_l[-1].start()
    for c in range(chunks):
        cols = pl.ds(c * cw, cw)
        loads_x.append(pltpu.make_async_copy(x_hbm.at[:, cols], x_buf.at[:, cols], x_sem.at[c]))
        loads_x[-1].start()
    is_relayed = relayed_ref[0] != 0
    act = jnp.zeros((x_buf.shape[0], rank), jnp.float32)
    p_in = jnp.where(is_relayed, p_in_ref[...].astype(jnp.float32), 0.0).astype(jnp.bfloat16)
    for c in range(chunks):
        cols = pl.ds(c * cw, cw)
        loads_l[c].wait()
        relayed = l_buf[:, cols].astype(jnp.float32) + jnp.dot(
            p_in, w_up_ref[:, cols], preferred_element_type=jnp.float32
        )
        incoming = relayed.astype(jnp.bfloat16)
        l_buf[:, cols] = incoming
        act = act + nt_dot(incoming, wout_ref[:, cols])
    pre = pre_ref[...]
    hidden_t = jax.nn.silu(pre).T.astype(jnp.bfloat16)
    grad = act * silu_slope(pre)
    p_now = grad.astype(jnp.bfloat16)
    p_t = grad.T.astype(jnp.bfloat16)
    stores = []
    for c in range(chunks):
        cols = pl.ds(c * cw, cw)
        loads_x[c].wait()
        incoming = l_buf[:, cols]
        o_buf[:, cols] = (
            incoming.astype(jnp.float32) + jnp.dot(p_now, win_ref[:, cols], preferred_element_type=jnp.float32)
        ).astype(jnp.bfloat16)
        for m in range(micro_count):
            store = pltpu.make_async_copy(
                o_buf.at[pl.ds(m * tok_rows, tok_rows), cols],
                out_hbm.at[slot_ref[m], :, cols],
                o_sem.at[c, m],
            )
            store.start()
            stores.append(store)
        gin[cols, :] = jnp.dot(p_t, x_buf[:, cols], preferred_element_type=jnp.float32).T
        gout[:, cols] = jnp.dot(hidden_t, incoming, preferred_element_type=jnp.float32)
    block_rows = q_ref.shape[1]
    tiles = width // 128
    for b in range(n // 2):
        start = b * block_rows * 2
        low = gin[pl.ds(start, block_rows, stride=2), :]
        high = gin[pl.ds(start + 1, block_rows, stride=2), :]
        q_ref[place_ref[b]] = jnp.concatenate([low, high], axis=1).astype(jnp.bfloat16)
    lines = block_rows // tiles
    for b in range(n // 2):
        for t in range(tiles):
            turn[pl.ds(t, lines, stride=tiles), :] = gout[b * lines : (b + 1) * lines, t * 128 : (t + 1) * 128]
        q_ref[place_ref[n // 2 + b]] = turn[...].astype(jnp.bfloat16)
    for store in stores:
        store.wait()


def drain(n, block_len, micro_count, relayed, slots, places, x, loss, pre, p_in, w_up, win, wout):
    rows, width = x.shape
    rank = win.shape[0]
    chunks = width // column_width(width)
    dma = pltpu.SemaphoreType.DMA
    return pl.pallas_call(
        functools.partial(drain_kernel, n),
        out_shape=(
            jax.ShapeDtypeStruct((micro_count, rows // micro_count, width), jnp.bfloat16),
            jax.ShapeDtypeStruct((n, block_len // 128, 128), jnp.bfloat16),
        ),
        in_specs=[SMEM, SMEM, SMEM, ANY, ANY, VMEM, VMEM, VMEM, VMEM, VMEM],
        out_specs=(ANY, VMEM),
        scratch_shapes=[
            pltpu.VMEM(x.shape, jnp.bfloat16),
            pltpu.VMEM(x.shape, jnp.bfloat16),
            pltpu.VMEM(x.shape, jnp.bfloat16),
            pltpu.VMEM((width, rank), jnp.float32),
            pltpu.VMEM((rank, width), jnp.float32),
            pltpu.VMEM((block_len // 128, 128), jnp.float32),
            dma((chunks,)), dma((chunks,)), dma((chunks, micro_count)),
        ],
        name="drain",
    )(relayed, slots, places, x, loss, pre, p_in, w_up, win, wout)


def reduce_kernel(
    n, q_ref, m_ref, v_ref, u_ref, first_ref, second_ref,
    near, summed, far, s1, r1, s2, r2,
):
    me = lax.axis_index("dp")
    core = lax.rem(me, 2)
    chip = me // 2
    chips = n // 2
    sibling = me + 1 - 2 * core
    greet(n, me, None)

    def near_copy(d):
        to = lax.rem(chip + d, chips)
        return pltpu.make_async_remote_copy(
            q_ref.at[(1 - core) * chips + to], near.at[to], s1.at[d], r1.at[d],
            device_id={"dp": sibling}, device_id_type=MESH,
        )

    def far_copy(d):
        to = lax.rem(chip + d, chips)
        return pltpu.make_async_remote_copy(
            summed.at[to], far.at[d], s2.at[d], r2.at[d],
            device_id={"dp": to * 2 + core}, device_id_type=MESH,
        )

    @pl.loop(1, chips + 1)
    def _(step):
        near_copy(lax.rem(step, chips)).start()

    @pl.loop(1, chips)
    def _(d):
        to = lax.rem(chip + d, chips)
        near_copy(d).wait_recv()
        summed[to] = (
            q_ref[core * chips + to].astype(jnp.float32) + near[to].astype(jnp.float32)
        ).astype(jnp.bfloat16)
        far_copy(d).start()

    near_copy(0).wait_recv()
    total = q_ref[core * chips + chip].astype(jnp.float32) + near[chip].astype(jnp.float32)
    first_ref[...] = total

    @pl.loop(1, chips)
    def _(d):
        far_copy(d).wait_recv()
        first_ref[...] += far[d].astype(jnp.float32)

    grads = first_ref[...] / loss_scale
    first_next = beta_one * m_ref[...] + (1.0 - beta_one) * grads
    second_next = beta_two * v_ref[...] + (1.0 - beta_two) * grads * grads
    first_ref[...] = first_next
    second_ref[...] = second_next
    u_ref[...] = (
        first_next
        / (1.0 - beta_one**adam_step)
        / (jnp.sqrt(second_next / (1.0 - beta_two**adam_step)) + adam_eps)
    )

    @pl.loop(0, chips)
    def _(d):
        near_copy(d).wait_send()

    @pl.loop(1, chips)
    def _(d):
        far_copy(d).wait_send()


def reduce_adam(n, blocks, m, v):
    lines = m.shape
    dma = pltpu.SemaphoreType.DMA
    shape = jax.ShapeDtypeStruct(lines, jnp.float32)
    group = pltpu.VMEM((n // 2,) + lines, jnp.bfloat16)
    return pl.pallas_call(
        functools.partial(reduce_kernel, n),
        out_shape=(shape,) * 3,
        in_specs=[VMEM] * 3,
        out_specs=(VMEM,) * 3,
        scratch_shapes=[group, group, group] + [dma((n // 2,))] * 4,
        compiler_params=pltpu.CompilerParams(collective_id=1, has_side_effects=True),
        name="reduce_adam",
    )(blocks, m, v)


def passed_along(value, axis, steps):
    count = lax.axis_size(axis)
    first, last = (max(0, -steps), min(count, count - steps))
    return lax.ppermute(value, axis, [(source, source + steps) for source in range(first, last)])


def silu_slope(pre_value):
    gate_value = jax.nn.sigmoid(pre_value)
    return gate_value * (1.0 + pre_value * (1.0 - gate_value))


def per_device(
    activations,
    loss_grads,
    adapter_in,
    adapter_out,
    first_moment,
    second_moment,
    old_owner,
    new_owner,
    plan,
):
    sections = lax.axis_size("section")
    section_index = lax.axis_index("section")
    replicas = lax.axis_size("dp")
    my_index = lax.axis_index("dp")
    weight_in = adapter_in[0]
    weight_out = adapter_out[0]
    inputs_all = activations[0]
    micro_count = inputs_all.shape[0]
    tok_rows = inputs_all.shape[1]
    width = inputs_all.shape[2]
    owners_old = old_owner[0]
    owners_new = new_owner[0]
    block_len = first_moment.shape[2] // 2
    replica_ids = jnp.arange(replicas, dtype=jnp.int32)
    new_block = jnp.sum(jnp.where(owners_new == my_index, replica_ids, 0))

    def drain_turn(turn_index, state):
        previous, grad_in, grad_out, emitted = state
        received = passed_along(previous, "section", -1)
        slot = turn_index - (sections - 1 - section_index)
        is_valid = (slot >= 0) & (slot < micro_count)
        clamped = jnp.clip(slot, 0, micro_count - 1)
        micro = lax.dynamic_index_in_dim(plan, clamped, 0, keepdims=False)
        section_input = lax.dynamic_index_in_dim(inputs_all, micro, 0, keepdims=False)
        from_loss = lax.dynamic_index_in_dim(loss_grads, micro, 0, keepdims=False)
        incoming = jnp.where(section_index == sections - 1, from_loss, received)
        pre_value = jnp.dot(section_input, weight_in, preferred_element_type=jnp.float32)
        hidden = jax.nn.silu(pre_value).astype(jnp.bfloat16)
        act_grad = jnp.dot(incoming, weight_out.T, preferred_element_type=jnp.float32)
        pre_grad = (act_grad * silu_slope(pre_value)).astype(jnp.bfloat16)
        input_grad = (
            incoming.astype(jnp.float32)
            + jnp.dot(pre_grad, weight_in.T, preferred_element_type=jnp.float32)
        ).astype(jnp.bfloat16)
        valid_weight = is_valid.astype(jnp.float32)
        grad_in = grad_in + valid_weight * jnp.dot(
            section_input.T, pre_grad, preferred_element_type=jnp.float32
        )
        grad_out = grad_out + valid_weight * jnp.dot(
            hidden.T, incoming, preferred_element_type=jnp.float32
        )
        earlier = lax.dynamic_index_in_dim(emitted, clamped, 0, keepdims=False)
        written = jnp.where(is_valid, input_grad, earlier)
        emitted = lax.dynamic_update_index_in_dim(emitted, written, clamped, 0)
        return (input_grad, grad_in, grad_out, emitted)

    start_state = (
        jnp.zeros((tok_rows, width), jnp.bfloat16),
        jnp.zeros(weight_in.shape, jnp.float32),
        jnp.zeros(weight_out.shape, jnp.float32),
        jnp.zeros((micro_count, tok_rows, width), jnp.bfloat16),
    )
    place_of_block = owners_new % 2 * (replicas // 2) + owners_new // 2
    lines = (block_len // 128, 128)
    if sections == 2:
        rows = micro_count * tok_rows
        flat_inputs = inputs_all.reshape(rows, width)
        flat_loss = loss_grads.reshape(rows, width)
        turned_in = weight_in.T
        piece_len = block_len // replicas
        lanes = math.gcd(2 * piece_len, 128)
        pieces = jnp.stack([first_moment[0, 0], second_moment[0, 0]]).astype(jnp.bfloat16)
        pieces = pieces.reshape(2, 2, replicas, piece_len).transpose(2, 1, 0, 3)
        pieces = pieces.reshape(replicas, 2, 2 * piece_len // lanes, lanes)
        block_of = jnp.sum(
            jnp.where(owners_new[None, :] == replica_ids[:, None], replica_ids[None, :], 0), axis=1
        )
        holder = owners_old[block_of // 2]
        picks = jnp.stack([holder, block_of % 2], axis=1)
        pre, p_up, w_up, got = exchange(
            replicas, flat_inputs, flat_loss, turned_in, weight_out, pieces, picks
        )
        slot_ids = jnp.arange(micro_count, dtype=jnp.int32)
        slots = jnp.sum(jnp.where(plan[None, :] == slot_ids[:, None], slot_ids[None, :], 0), axis=1)
        relayed = (section_index < sections - 1).astype(jnp.int32).reshape(1)
        emitted, blocks = drain(
            replicas, block_len, micro_count, relayed, slots, place_of_block,
            flat_inputs, flat_loss, pre, p_up, w_up, turned_in, weight_out,
        )
        got = got.reshape(replicas, 2, piece_len).astype(jnp.float32)
        first_old, second_old = (got[:, 0].reshape(lines), got[:, 1].reshape(lines))
        update, first_next, second_next = reduce_adam(replicas, blocks, first_old, second_old)
        shape = (1, 1, block_len)
        return (emitted[None], update.reshape(shape), first_next.reshape(shape), second_next.reshape(shape))
    last_grad, grad_in, grad_out, emitted = lax.fori_loop(
        0, micro_count + sections - 1, drain_turn, start_state
    )
    partial_value = jnp.concatenate([grad_in.reshape(-1), grad_out.reshape(-1)])
    block_at = jnp.sum(
        jnp.where(place_of_block[None, :] == replica_ids[:, None], replica_ids[None, :], 0), axis=1
    )
    blocks = jnp.take(partial_value.astype(jnp.bfloat16).reshape((replicas,) + lines), block_at, axis=0)
    old_count = owners_old.shape[0]
    piece_len = 2 * block_len // replicas
    first_pieces = first_moment[0, 0].reshape(replicas, piece_len)
    second_pieces = second_moment[0, 0].reshape(replicas, piece_len)
    first_spread = lax.all_to_all(first_pieces, "dp", split_axis=0, concat_axis=0, tiled=True)
    second_spread = lax.all_to_all(second_pieces, "dp", split_axis=0, concat_axis=0, tiled=True)
    first_held = jnp.take(first_spread, owners_old, axis=0)
    second_held = jnp.take(second_spread, owners_old, axis=0)
    my_half = my_index // old_count
    targets = owners_new.reshape(-1, 2)
    target_of_block = jnp.where(my_half == 0, targets[:, 0], targets[:, 1])
    picker = (target_of_block[None, :] == replica_ids[:, None]).astype(jnp.float32)
    first_out = jnp.dot(picker, first_held, precision=lax.Precision.HIGHEST)
    second_out = jnp.dot(picker, second_held, precision=lax.Precision.HIGHEST)
    first_got = lax.all_to_all(first_out, "dp", split_axis=0, concat_axis=0, tiled=True)
    second_got = lax.all_to_all(second_out, "dp", split_axis=0, concat_axis=0, tiled=True)
    half_start = new_block % 2 * old_count
    first_mine = lax.dynamic_slice_in_dim(first_got, half_start, old_count, 0).reshape(-1)
    second_mine = lax.dynamic_slice_in_dim(second_got, half_start, old_count, 0).reshape(-1)
    update, first_next, second_next = reduce_adam(
        replicas, blocks, first_mine.reshape(lines), second_mine.reshape(lines)
    )
    shape = (1, 1, block_len)
    return (emitted[None], update.reshape(shape), first_next.reshape(shape), second_next.reshape(shape))


def solution(mesh):
    placed = (
        P("section", None, "dp", None),
        P(None, "dp", None),
        P("section", None, None),
        P("section", None, None),
        P("section", "dp", None),
        P("section", "dp", None),
        P("section", None),
        P("section", None),
        P(),
    )
    return jax.shard_map(
        per_device,
        mesh=mesh,
        in_specs=placed,
        out_specs=(
            P("section", None, "dp", None),
            P("section", "dp", None),
            P("section", "dp", None),
            P("section", "dp", None),
        ),
        check_vma=False,
    )
```

```python
import functools
import math

import jax
import jax.numpy as jnp
from jax import lax
from jax.experimental import pallas as pl
from jax.experimental.pallas import tpu as pltpu
from jax.sharding import PartitionSpec as P

beta_one = 0.9
beta_two = 0.95
adam_eps = 1e-08
adam_step = 1000.0
loss_scale = 4096.0
MESH = pl.DeviceIdType.MESH
VMEM = pl.BlockSpec(memory_space=pltpu.VMEM)
SMEM = pl.BlockSpec(memory_space=pltpu.SMEM)
ANY = pl.BlockSpec(memory_space=pl.ANY)


def nt_dot(left, right):
    return lax.dot_general(left, right, (((1,), (1,)), ((), ())), preferred_element_type=jnp.float32)


def column_width(width):
    return 128 * max(d for d in range(1, 8) if (width // 128) % d == 0)


def greet(n, me, extra):
    barrier = pltpu.get_barrier_semaphore()

    @pl.loop(1, n)
    def _(d):
        pl.semaphore_signal(barrier, inc=1, device_id={"dp": lax.rem(me + d, n)}, device_id_type=MESH)

    if extra is not None:
        pl.semaphore_signal(barrier, inc=1, device_id={"section": extra}, device_id_type=MESH)
    pl.semaphore_wait(barrier, n - 1 + (extra is not None))


def relay_kernel(
    n, block_rows, new_ref, old_ref, x_hbm, l_hbm, win_ref, wout_ref, m_ref, v_ref,
    p_up_ref, w_ref, p_ref, total_ref, first_ref, second_ref,
    order, x_buf, l_buf, p_buf, pieces, spread, chosen, got, gin, gout, turn,
    blocks, outbox, near, summed, far,
    x_sem, l_sem, w_send, w_recv, f_send, f_recv, p_send, p_recv, a_send, a_recv, b_send, b_recv, own_sem,
    s1, r1, s2, r2,
):
    me = lax.axis_index("dp")
    section = lax.axis_index("section")
    other = 1 - section
    core = lax.rem(me, 2)
    sibling = me + 1 - 2 * core
    chip = me // 2
    chips = n // 2
    rank, width = win_ref.shape
    cw = column_width(width)
    chunks = width // cw
    loads = []
    for c in range(chunks):
        cols = pl.ds(c * cw, cw)
        for src, dst, sem in ((x_hbm, x_buf, x_sem), (l_hbm, l_buf, l_sem)):
            load = pltpu.make_async_copy(src.at[:, cols], dst.at[:, cols], sem.at[c])
            load.start()
            loads.append(load)
    barrier = pltpu.get_barrier_semaphore()

    @pl.loop(1, n)
    def _(d):
        pl.semaphore_signal(barrier, inc=1, device_id={"dp": lax.rem(me + d, n)}, device_id_type=MESH)

    pl.semaphore_signal(barrier, inc=1, device_id={"section": other}, device_id_type=MESH)
    part = block_rows // n
    slab = pieces.shape[2] // 2
    filler = [jnp.zeros((slab - part, 128), jnp.float32)] if slab > part else []
    for t in range(n):
        for h in range(2):
            start = h * block_rows + t * part
            pieces[t, h] = jnp.concatenate(
                [m_ref[start : start + part, :]] + filler + [v_ref[start : start + part, :]] + filler, axis=0
            ).astype(jnp.bfloat16)
    pl.semaphore_wait(barrier, n)
    half = rank // 2
    mine = pl.ds(pl.multiple_of(core * half, half), half)
    theirs = pl.ds(pl.multiple_of((1 - core) * half, half), half)
    w_copy = pltpu.make_async_remote_copy(
        win_ref.at[mine], w_ref.at[mine], w_send, w_recv, device_id={"section": other}, device_id_type=MESH
    )
    w_copy.start()

    def spread_copy(d):
        peer = lax.rem(me + d, n)
        return pltpu.make_async_remote_copy(
            pieces.at[peer], spread.at[me], a_send.at[d], a_recv.at[d],
            device_id={"dp": peer}, device_id_type=MESH,
        )

    def spread_arrival(d):
        peer = lax.rem(me + n - d, n)
        return pltpu.make_async_remote_copy(
            pieces.at[peer], spread.at[peer], a_send.at[d], a_recv.at[d],
            device_id={"dp": peer}, device_id_type=MESH,
        )

    def gather_copy(d):
        peer = lax.rem(me + d, n)
        return pltpu.make_async_remote_copy(
            chosen.at[peer], got.at[me], b_send.at[d], b_recv.at[d],
            device_id={"dp": peer}, device_id_type=MESH,
        )

    def gather_arrival(d):
        peer = lax.rem(me + n - d, n)
        return pltpu.make_async_remote_copy(
            chosen.at[peer], got.at[peer], b_send.at[d], b_recv.at[d],
            device_id={"dp": peer}, device_id_type=MESH,
        )

    @pl.loop(1, n)
    def _(d):
        spread_copy(d).start()

    own = pltpu.make_async_copy(pieces.at[me], spread.at[me], own_sem.at[0])
    own.start()
    owners = [new_ref[c] for c in range(n)]
    for t in range(n):
        block = jnp.int32(0)
        for c in range(1, n):
            block = jnp.where(owners[c] == t, c, block)
        order[t] = block

    rows = x_buf.shape[0]
    pre = jnp.zeros((rows, rank), jnp.float32)
    act = jnp.zeros((rows, rank), jnp.float32)
    for c in range(chunks):
        cols = pl.ds(c * cw, cw)
        loads[2 * c].wait()
        loads[2 * c + 1].wait()
        pre = pre + nt_dot(x_buf[:, cols], win_ref[:, cols])
        act = act + nt_dot(l_buf[:, cols], wout_ref[:, cols])
    slope = silu_slope(pre)
    p_buf[...] = (act * slope).astype(jnp.bfloat16)
    p_copy = pltpu.make_async_remote_copy(
        p_buf, p_up_ref, p_send, p_recv, device_id={"section": other}, device_id_type=MESH
    )
    p_copy.start()
    hidden_t = jax.nn.silu(pre).T.astype(jnp.bfloat16)
    w_copy.wait_recv()
    forward = pltpu.make_async_remote_copy(
        w_ref.at[mine], w_ref.at[mine], f_send, f_recv, device_id={"dp": sibling}, device_id_type=MESH
    )
    forward.start()
    pltpu.make_async_remote_copy(
        w_ref.at[theirs], w_ref.at[theirs], f_send, f_recv, device_id={"dp": sibling}, device_id_type=MESH
    ).wait_recv()
    p_copy.wait_recv()
    p_in = jnp.where(section == 0, p_up_ref[...].astype(jnp.float32), 0.0).astype(jnp.bfloat16)
    act = jnp.zeros((rows, rank), jnp.float32)
    for c in range(chunks):
        cols = pl.ds(c * cw, cw)
        incoming = (
            l_buf[:, cols].astype(jnp.float32)
            + jnp.dot(p_in, w_ref[:, cols], preferred_element_type=jnp.float32)
        ).astype(jnp.bfloat16)
        act = act + nt_dot(incoming, wout_ref[:, cols])
        gout[:, cols] = jnp.dot(hidden_t, incoming, preferred_element_type=jnp.float32)
    grad = act * slope
    p_ref[...] = grad.astype(jnp.bfloat16)
    p_t = grad.T.astype(jnp.bfloat16)
    own.wait()

    @pl.loop(1, n)
    def _(d):
        spread_arrival(d).wait_recv()

    for t in range(n):
        block = order[t]
        chosen[t] = spread[old_ref[block // 2], lax.rem(block, 2)]

    @pl.loop(1, n)
    def _(d):
        gather_copy(d).start()

    keep = pltpu.make_async_copy(chosen.at[me], got.at[me], own_sem.at[1])
    keep.start()
    for c in range(chunks):
        cols = pl.ds(c * cw, cw)
        gin[cols, :] = jnp.dot(p_t, x_buf[:, cols], preferred_element_type=jnp.float32).T
    tiles = width // 128
    lines = block_rows // tiles
    for b in range(chips):
        start = b * block_rows * 2
        low = gin[pl.ds(start, block_rows, stride=2), :]
        high = gin[pl.ds(start + 1, block_rows, stride=2), :]
        blocks[b] = jnp.concatenate([low, high], axis=1).astype(jnp.bfloat16)
    for b in range(chips):
        for t in range(tiles):
            turn[pl.ds(t, lines, stride=tiles), :] = gout[b * lines : (b + 1) * lines, t * 128 : (t + 1) * 128]
        blocks[chips + b] = turn[...].astype(jnp.bfloat16)

    def near_copy(d):
        to = lax.rem(chip + d, chips)
        return pltpu.make_async_remote_copy(
            outbox.at[to], near.at[to], s1.at[d], r1.at[d], device_id={"dp": sibling}, device_id_type=MESH
        )

    def far_copy(d):
        to = lax.rem(chip + d, chips)
        return pltpu.make_async_remote_copy(
            summed.at[to], far.at[d], s2.at[d], r2.at[d],
            device_id={"dp": to * 2 + core}, device_id_type=MESH,
        )

    @pl.loop(1, chips + 1)
    def _(step):
        to = lax.rem(chip + step, chips)
        outbox[to] = blocks[order[to * 2 + 1 - core]]
        near_copy(lax.rem(step, chips)).start()

    @pl.loop(1, chips)
    def _(d):
        to = lax.rem(chip + d, chips)
        near_copy(d).wait_recv()
        summed[to] = (
            blocks[order[to * 2 + core]].astype(jnp.float32) + near[to].astype(jnp.float32)
        ).astype(jnp.bfloat16)
        far_copy(d).start()

    near_copy(0).wait_recv()
    total_ref[...] = blocks[order[me]].astype(jnp.float32) + near[chip].astype(jnp.float32)
    keep.wait()

    @pl.loop(1, n)
    def _(d):
        gather_arrival(d).wait_recv()

    for t in range(n):
        place = pl.ds(t * part, part)
        held = got[t].astype(jnp.float32)
        first_ref[place, :] = held[:part, :]
        second_ref[place, :] = held[slab : slab + part, :]

    @pl.loop(1, chips)
    def _(d):
        far_copy(d).wait_recv()
        total_ref[...] += far[d].astype(jnp.float32)

    w_copy.wait_send()
    p_copy.wait_send()
    forward.wait_send()

    @pl.loop(1, n)
    def _(d):
        spread_copy(d).wait_send()
        gather_copy(d).wait_send()

    @pl.loop(0, chips)
    def _(d):
        near_copy(d).wait_send()

    @pl.loop(1, chips)
    def _(d):
        far_copy(d).wait_send()


def relay(n, new_owner, old_owner, x, loss, win, wout, first, second):
    rows, width = x.shape
    rank = win.shape[0]
    chunks = width // column_width(width)
    block_rows = first.shape[0] // 2
    slab = -(-(block_rows // n) // 8) * 8
    dma = pltpu.SemaphoreType.DMA
    bf16, f32 = jnp.bfloat16, jnp.float32
    group = pltpu.VMEM((n // 2, block_rows, 128), bf16)
    lines = jax.ShapeDtypeStruct((block_rows, 128), f32)
    return pl.pallas_call(
        functools.partial(relay_kernel, n, block_rows),
        out_shape=(
            jax.ShapeDtypeStruct((rows, rank), bf16),
            jax.ShapeDtypeStruct((rank, width), bf16),
            jax.ShapeDtypeStruct((rows, rank), bf16),
            lines, lines, lines,
        ),
        in_specs=[SMEM, SMEM, ANY, ANY, VMEM, VMEM, VMEM, VMEM],
        out_specs=(VMEM,) * 6,
        scratch_shapes=[
            pltpu.SMEM((n,), jnp.int32),
            pltpu.VMEM(x.shape, bf16),
            pltpu.VMEM(x.shape, bf16),
            pltpu.VMEM((rows, rank), bf16),
            pltpu.VMEM((n, 2, 2 * slab, 128), bf16),
            pltpu.VMEM((n, 2, 2 * slab, 128), bf16),
            pltpu.VMEM((n, 2 * slab, 128), bf16),
            pltpu.VMEM((n, 2 * slab, 128), bf16),
            pltpu.VMEM((width, rank), f32),
            pltpu.VMEM((rank, width), f32),
            pltpu.VMEM((block_rows, 128), f32),
            pltpu.VMEM((n, block_rows, 128), bf16),
            group, group, group, group,
            dma((chunks,)), dma((chunks,)), dma, dma, dma, dma, dma, dma,
            dma((n,)), dma((n,)), dma((n,)), dma((n,)), dma((2,)),
            dma((n // 2,)), dma((n // 2,)), dma((n // 2,)), dma((n // 2,)),
        ],
        compiler_params=pltpu.CompilerParams(collective_id=0, has_side_effects=True),
        name="relay",
    )(new_owner, old_owner, x, loss, win, wout, first, second)


def emit_kernel(
    relayed_ref, slot_ref, l_hbm, p_up_ref, w_up_ref, p_ref, win_ref, total_ref, m_ref, v_ref,
    out_hbm, u_ref, first_ref, second_ref,
    l_buf, o_buf, l_sem, o_sem,
):
    rank, width = win_ref.shape
    micro_count, tok_rows, _ = out_hbm.shape
    cw = column_width(width)
    chunks = width // cw
    loads = []
    for c in range(chunks):
        cols = pl.ds(c * cw, cw)
        loads.append(pltpu.make_async_copy(l_hbm.at[:, cols], l_buf.at[:, cols], l_sem.at[c]))
        loads[-1].start()
    adam(total_ref[...], m_ref[...], v_ref[...], u_ref, first_ref, second_ref)
    is_relayed = relayed_ref[0] != 0
    p_up = jnp.where(is_relayed, p_up_ref[...].astype(jnp.float32), 0.0).astype(jnp.bfloat16)
    p_now = p_ref[...]
    stores = []
    for c in range(chunks):
        cols = pl.ds(c * cw, cw)
        loads[c].wait()
        incoming = (
            l_buf[:, cols].astype(jnp.float32)
            + jnp.dot(p_up, w_up_ref[:, cols], preferred_element_type=jnp.float32)
        ).astype(jnp.bfloat16)
        o_buf[:, cols] = (
            incoming.astype(jnp.float32) + jnp.dot(p_now, win_ref[:, cols], preferred_element_type=jnp.float32)
        ).astype(jnp.bfloat16)
        for m in range(micro_count):
            store = pltpu.make_async_copy(
                o_buf.at[pl.ds(m * tok_rows, tok_rows), cols],
                out_hbm.at[slot_ref[m], :, cols],
                o_sem.at[c, m],
            )
            store.start()
            stores.append(store)
    for store in stores:
        store.wait()


def emit(micro_count, relayed, slots, loss, p_up, w_up, p_now, win, total, m, v):
    rows, width = loss.shape
    chunks = width // column_width(width)
    dma = pltpu.SemaphoreType.DMA
    lines = jax.ShapeDtypeStruct(m.shape, jnp.float32)
    return pl.pallas_call(
        emit_kernel,
        out_shape=(
            jax.ShapeDtypeStruct((micro_count, rows // micro_count, width), jnp.bfloat16),
            lines, lines, lines,
        ),
        in_specs=[SMEM, SMEM, ANY] + [VMEM] * 7,
        out_specs=(ANY, VMEM, VMEM, VMEM),
        scratch_shapes=[
            pltpu.VMEM(loss.shape, jnp.bfloat16),
            pltpu.VMEM(loss.shape, jnp.bfloat16),
            dma((chunks,)), dma((chunks, micro_count)),
        ],
        name="emit",
    )(relayed, slots, loss, p_up, w_up, p_now, win, total, m, v)


def adam(total, m, v, u_ref, first_ref, second_ref):
    grads = total / loss_scale
    first_next = beta_one * m + (1.0 - beta_one) * grads
    second_next = beta_two * v + (1.0 - beta_two) * grads * grads
    first_ref[...] = first_next
    second_ref[...] = second_next
    u_ref[...] = (
        first_next
        / (1.0 - beta_one**adam_step)
        / (jnp.sqrt(second_next / (1.0 - beta_two**adam_step)) + adam_eps)
    )


def reduce_kernel(
    n, q_ref, m_ref, v_ref, u_ref, first_ref, second_ref,
    near, summed, far, s1, r1, s2, r2,
):
    me = lax.axis_index("dp")
    core = lax.rem(me, 2)
    chip = me // 2
    chips = n // 2
    sibling = me + 1 - 2 * core
    greet(n, me, None)

    def near_copy(d):
        to = lax.rem(chip + d, chips)
        return pltpu.make_async_remote_copy(
            q_ref.at[(1 - core) * chips + to], near.at[to], s1.at[d], r1.at[d],
            device_id={"dp": sibling}, device_id_type=MESH,
        )

    def far_copy(d):
        to = lax.rem(chip + d, chips)
        return pltpu.make_async_remote_copy(
            summed.at[to], far.at[d], s2.at[d], r2.at[d],
            device_id={"dp": to * 2 + core}, device_id_type=MESH,
        )

    @pl.loop(1, chips + 1)
    def _(step):
        near_copy(lax.rem(step, chips)).start()

    @pl.loop(1, chips)
    def _(d):
        to = lax.rem(chip + d, chips)
        near_copy(d).wait_recv()
        summed[to] = (
            q_ref[core * chips + to].astype(jnp.float32) + near[to].astype(jnp.float32)
        ).astype(jnp.bfloat16)
        far_copy(d).start()

    near_copy(0).wait_recv()
    total = q_ref[core * chips + chip].astype(jnp.float32) + near[chip].astype(jnp.float32)
    first_ref[...] = total

    @pl.loop(1, chips)
    def _(d):
        far_copy(d).wait_recv()
        first_ref[...] += far[d].astype(jnp.float32)

    adam(first_ref[...], m_ref[...], v_ref[...], u_ref, first_ref, second_ref)

    @pl.loop(0, chips)
    def _(d):
        near_copy(d).wait_send()

    @pl.loop(1, chips)
    def _(d):
        far_copy(d).wait_send()


def reduce_adam(n, blocks, m, v):
    lines = m.shape
    dma = pltpu.SemaphoreType.DMA
    shape = jax.ShapeDtypeStruct(lines, jnp.float32)
    group = pltpu.VMEM((n // 2,) + lines, jnp.bfloat16)
    return pl.pallas_call(
        functools.partial(reduce_kernel, n),
        out_shape=(shape,) * 3,
        in_specs=[VMEM] * 3,
        out_specs=(VMEM,) * 3,
        scratch_shapes=[group, group, group] + [dma((n // 2,))] * 4,
        compiler_params=pltpu.CompilerParams(collective_id=1, has_side_effects=True),
        name="reduce_adam",
    )(blocks, m, v)


def passed_along(value, axis, steps):
    count = lax.axis_size(axis)
    first, last = (max(0, -steps), min(count, count - steps))
    return lax.ppermute(value, axis, [(source, source + steps) for source in range(first, last)])


def silu_slope(pre_value):
    gate_value = jax.nn.sigmoid(pre_value)
    return gate_value * (1.0 + pre_value * (1.0 - gate_value))


def per_device(
    activations,
    loss_grads,
    adapter_in,
    adapter_out,
    first_moment,
    second_moment,
    old_owner,
    new_owner,
    plan,
):
    sections = lax.axis_size("section")
    section_index = lax.axis_index("section")
    replicas = lax.axis_size("dp")
    my_index = lax.axis_index("dp")
    weight_in = adapter_in[0]
    weight_out = adapter_out[0]
    inputs_all = activations[0]
    micro_count = inputs_all.shape[0]
    tok_rows = inputs_all.shape[1]
    width = inputs_all.shape[2]
    owners_old = old_owner[0]
    owners_new = new_owner[0]
    block_len = first_moment.shape[2] // 2
    replica_ids = jnp.arange(replicas, dtype=jnp.int32)
    new_block = jnp.sum(jnp.where(owners_new == my_index, replica_ids, 0))

    def drain_turn(turn_index, state):
        previous, grad_in, grad_out, emitted = state
        received = passed_along(previous, "section", -1)
        slot = turn_index - (sections - 1 - section_index)
        is_valid = (slot >= 0) & (slot < micro_count)
        clamped = jnp.clip(slot, 0, micro_count - 1)
        micro = lax.dynamic_index_in_dim(plan, clamped, 0, keepdims=False)
        section_input = lax.dynamic_index_in_dim(inputs_all, micro, 0, keepdims=False)
        from_loss = lax.dynamic_index_in_dim(loss_grads, micro, 0, keepdims=False)
        incoming = jnp.where(section_index == sections - 1, from_loss, received)
        pre_value = jnp.dot(section_input, weight_in, preferred_element_type=jnp.float32)
        hidden = jax.nn.silu(pre_value).astype(jnp.bfloat16)
        act_grad = jnp.dot(incoming, weight_out.T, preferred_element_type=jnp.float32)
        pre_grad = (act_grad * silu_slope(pre_value)).astype(jnp.bfloat16)
        input_grad = (
            incoming.astype(jnp.float32)
            + jnp.dot(pre_grad, weight_in.T, preferred_element_type=jnp.float32)
        ).astype(jnp.bfloat16)
        valid_weight = is_valid.astype(jnp.float32)
        grad_in = grad_in + valid_weight * jnp.dot(
            section_input.T, pre_grad, preferred_element_type=jnp.float32
        )
        grad_out = grad_out + valid_weight * jnp.dot(
            hidden.T, incoming, preferred_element_type=jnp.float32
        )
        earlier = lax.dynamic_index_in_dim(emitted, clamped, 0, keepdims=False)
        written = jnp.where(is_valid, input_grad, earlier)
        emitted = lax.dynamic_update_index_in_dim(emitted, written, clamped, 0)
        return (input_grad, grad_in, grad_out, emitted)

    start_state = (
        jnp.zeros((tok_rows, width), jnp.bfloat16),
        jnp.zeros(weight_in.shape, jnp.float32),
        jnp.zeros(weight_out.shape, jnp.float32),
        jnp.zeros((micro_count, tok_rows, width), jnp.bfloat16),
    )
    place_of_block = owners_new % 2 * (replicas // 2) + owners_new // 2
    lines = (block_len // 128, 128)
    if sections == 2 and replicas % 2 == 0 and block_len % (128 * replicas) == 0:
        rows = micro_count * tok_rows
        flat_inputs = inputs_all.reshape(rows, width)
        flat_loss = loss_grads.reshape(rows, width)
        turned_in = weight_in.T
        row_lines = (2 * block_len // 128, 128)
        p_up, w_up, p_now, total, first_old, second_old = relay(
            replicas, owners_new, owners_old, flat_inputs, flat_loss, turned_in, weight_out,
            first_moment.reshape(row_lines), second_moment.reshape(row_lines),
        )
        slot_ids = jnp.arange(micro_count, dtype=jnp.int32)
        slots = jnp.sum(jnp.where(plan[None, :] == slot_ids[:, None], slot_ids[None, :], 0), axis=1)
        relayed = (section_index < sections - 1).astype(jnp.int32).reshape(1)
        emitted, update, first_next, second_next = emit(
            micro_count, relayed, slots, flat_loss, p_up, w_up, p_now, turned_in, total, first_old, second_old
        )
        shape = (1, 1, block_len)
        return (emitted[None], update.reshape(shape), first_next.reshape(shape), second_next.reshape(shape))
    last_grad, grad_in, grad_out, emitted = lax.fori_loop(
        0, micro_count + sections - 1, drain_turn, start_state
    )
    partial_value = jnp.concatenate([grad_in.reshape(-1), grad_out.reshape(-1)])
    block_at = jnp.sum(
        jnp.where(place_of_block[None, :] == replica_ids[:, None], replica_ids[None, :], 0), axis=1
    )
    blocks = jnp.take(partial_value.astype(jnp.bfloat16).reshape((replicas,) + lines), block_at, axis=0)
    old_count = owners_old.shape[0]
    piece_len = 2 * block_len // replicas
    first_pieces = first_moment[0, 0].reshape(replicas, piece_len)
    second_pieces = second_moment[0, 0].reshape(replicas, piece_len)
    first_spread = lax.all_to_all(first_pieces, "dp", split_axis=0, concat_axis=0, tiled=True)
    second_spread = lax.all_to_all(second_pieces, "dp", split_axis=0, concat_axis=0, tiled=True)
    first_held = jnp.take(first_spread, owners_old, axis=0)
    second_held = jnp.take(second_spread, owners_old, axis=0)
    my_half = my_index // old_count
    targets = owners_new.reshape(-1, 2)
    target_of_block = jnp.where(my_half == 0, targets[:, 0], targets[:, 1])
    picker = (target_of_block[None, :] == replica_ids[:, None]).astype(jnp.float32)
    first_out = jnp.dot(picker, first_held, precision=lax.Precision.HIGHEST)
    second_out = jnp.dot(picker, second_held, precision=lax.Precision.HIGHEST)
    first_got = lax.all_to_all(first_out, "dp", split_axis=0, concat_axis=0, tiled=True)
    second_got = lax.all_to_all(second_out, "dp", split_axis=0, concat_axis=0, tiled=True)
    half_start = new_block % 2 * old_count
    first_mine = lax.dynamic_slice_in_dim(first_got, half_start, old_count, 0).reshape(-1)
    second_mine = lax.dynamic_slice_in_dim(second_got, half_start, old_count, 0).reshape(-1)
    update, first_next, second_next = reduce_adam(
        replicas, blocks, first_mine.reshape(lines), second_mine.reshape(lines)
    )
    shape = (1, 1, block_len)
    return (emitted[None], update.reshape(shape), first_next.reshape(shape), second_next.reshape(shape))


def solution(mesh):
    placed = (
        P("section", None, "dp", None),
        P(None, "dp", None),
        P("section", None, None),
        P("section", None, None),
        P("section", "dp", None),
        P("section", "dp", None),
        P("section", None),
        P("section", None),
        P(),
    )
    return jax.shard_map(
        per_device,
        mesh=mesh,
        in_specs=placed,
        out_specs=(
            P("section", None, "dp", None),
            P("section", "dp", None),
            P("section", "dp", None),
            P("section", "dp", None),
        ),
        check_vma=False,
    )
```

```python
import functools
import math

import jax
import jax.numpy as jnp
from jax import lax
from jax.experimental import pallas as pl
from jax.experimental.pallas import tpu as pltpu
from jax.sharding import PartitionSpec as P

beta_one = 0.9
beta_two = 0.95
adam_eps = 1e-08
adam_step = 1000.0
loss_scale = 4096.0
MESH = pl.DeviceIdType.MESH
VMEM = pl.BlockSpec(memory_space=pltpu.VMEM)
SMEM = pl.BlockSpec(memory_space=pltpu.SMEM)
ANY = pl.BlockSpec(memory_space=pl.ANY)


def nt_dot(left, right):
    return lax.dot_general(left, right, (((1,), (1,)), ((), ())), preferred_element_type=jnp.float32)


def column_width(width):
    return 128 * max(d for d in range(1, 8) if (width // 128) % d == 0)


def greet(n, me, extra):
    barrier = pltpu.get_barrier_semaphore()

    @pl.loop(1, n)
    def _(d):
        pl.semaphore_signal(barrier, inc=1, device_id={"dp": lax.rem(me + d, n)}, device_id_type=MESH)

    if extra is not None:
        pl.semaphore_signal(barrier, inc=1, device_id={"section": extra}, device_id_type=MESH)
    pl.semaphore_wait(barrier, n - 1 + (extra is not None))


def relay_kernel(
    n, block_rows, new_ref, old_ref, x_hbm, l_hbm, win_ref, wout_ref, m_ref, v_ref,
    p_up_ref, w_ref, p_ref, total_ref, first_ref, second_ref,
    order, x_buf, l_buf, p_buf, pieces, spread, chosen, got, gin, gout, turn,
    blocks, outbox, near, summed, mid, far,
    x_sem, l_sem, w_send, w_recv, f_send, f_recv, p_send, p_recv, a_send, a_recv, b_send, b_recv, own_sem,
    s1, r1, s2, r2, s3, r3,
):
    me = lax.axis_index("dp")
    section = lax.axis_index("section")
    other = 1 - section
    core = lax.rem(me, 2)
    sibling = me + 1 - 2 * core
    chip = me // 2
    chips = n // 2
    rank, width = win_ref.shape
    cw = column_width(width)
    chunks = width // cw
    loads = []
    for c in range(chunks):
        cols = pl.ds(c * cw, cw)
        for src, dst, sem in ((x_hbm, x_buf, x_sem), (l_hbm, l_buf, l_sem)):
            load = pltpu.make_async_copy(src.at[:, cols], dst.at[:, cols], sem.at[c])
            load.start()
            loads.append(load)
    barrier = pltpu.get_barrier_semaphore()

    @pl.loop(1, n)
    def _(d):
        pl.semaphore_signal(barrier, inc=1, device_id={"dp": lax.rem(me + d, n)}, device_id_type=MESH)

    pl.semaphore_signal(barrier, inc=1, device_id={"section": other}, device_id_type=MESH)
    part = block_rows // n
    slab = pieces.shape[2] // 2
    filler = [jnp.zeros((slab - part, 128), jnp.float32)] if slab > part else []
    for t in range(n):
        for h in range(2):
            start = h * block_rows + t * part
            pieces[t, h] = jnp.concatenate(
                [m_ref[start : start + part, :]] + filler + [v_ref[start : start + part, :]] + filler, axis=0
            ).astype(jnp.bfloat16)
    pl.semaphore_wait(barrier, n)
    half = rank // 2
    mine = pl.ds(pl.multiple_of(core * half, half), half)
    theirs = pl.ds(pl.multiple_of((1 - core) * half, half), half)
    w_copy = pltpu.make_async_remote_copy(
        win_ref.at[mine], w_ref.at[mine], w_send, w_recv, device_id={"section": other}, device_id_type=MESH
    )
    w_copy.start()

    def spread_copy(d):
        peer = lax.rem(me + d, n)
        return pltpu.make_async_remote_copy(
            pieces.at[peer], spread.at[me], a_send.at[d], a_recv.at[d],
            device_id={"dp": peer}, device_id_type=MESH,
        )

    def spread_arrival(d):
        peer = lax.rem(me + n - d, n)
        return pltpu.make_async_remote_copy(
            pieces.at[peer], spread.at[peer], a_send.at[d], a_recv.at[d],
            device_id={"dp": peer}, device_id_type=MESH,
        )

    def gather_copy(d):
        peer = lax.rem(me + d, n)
        return pltpu.make_async_remote_copy(
            chosen.at[peer], got.at[me], b_send.at[d], b_recv.at[d],
            device_id={"dp": peer}, device_id_type=MESH,
        )

    def gather_arrival(d):
        peer = lax.rem(me + n - d, n)
        return pltpu.make_async_remote_copy(
            chosen.at[peer], got.at[peer], b_send.at[d], b_recv.at[d],
            device_id={"dp": peer}, device_id_type=MESH,
        )

    @pl.loop(1, n)
    def _(d):
        spread_copy(d).start()

    own = pltpu.make_async_copy(pieces.at[me], spread.at[me], own_sem.at[0])
    own.start()
    owners = [new_ref[c] for c in range(n)]
    for t in range(n):
        block = jnp.int32(0)
        for c in range(1, n):
            block = jnp.where(owners[c] == t, c, block)
        order[t] = block

    rows = x_buf.shape[0]
    pre = jnp.zeros((rows, rank), jnp.float32)
    act = jnp.zeros((rows, rank), jnp.float32)
    for c in range(chunks):
        cols = pl.ds(c * cw, cw)
        loads[2 * c].wait()
        loads[2 * c + 1].wait()
        pre = pre + nt_dot(x_buf[:, cols], win_ref[:, cols])
        act = act + nt_dot(l_buf[:, cols], wout_ref[:, cols])
    slope = silu_slope(pre)
    p_buf[...] = (act * slope).astype(jnp.bfloat16)
    p_copy = pltpu.make_async_remote_copy(
        p_buf, p_up_ref, p_send, p_recv, device_id={"section": other}, device_id_type=MESH
    )
    p_copy.start()
    hidden_t = jax.nn.silu(pre).T.astype(jnp.bfloat16)
    w_copy.wait_recv()
    forward = pltpu.make_async_remote_copy(
        w_ref.at[mine], w_ref.at[mine], f_send, f_recv, device_id={"dp": sibling}, device_id_type=MESH
    )
    forward.start()
    pltpu.make_async_remote_copy(
        w_ref.at[theirs], w_ref.at[theirs], f_send, f_recv, device_id={"dp": sibling}, device_id_type=MESH
    ).wait_recv()
    p_copy.wait_recv()
    p_in = jnp.where(section == 0, p_up_ref[...].astype(jnp.float32), 0.0).astype(jnp.bfloat16)
    act = jnp.zeros((rows, rank), jnp.float32)
    for c in range(chunks):
        cols = pl.ds(c * cw, cw)
        incoming = (
            l_buf[:, cols].astype(jnp.float32)
            + jnp.dot(p_in, w_ref[:, cols], preferred_element_type=jnp.float32)
        ).astype(jnp.bfloat16)
        act = act + nt_dot(incoming, wout_ref[:, cols])
        gout[:, cols] = jnp.dot(hidden_t, incoming, preferred_element_type=jnp.float32)
    grad = act * slope
    p_ref[...] = grad.astype(jnp.bfloat16)
    p_t = grad.T.astype(jnp.bfloat16)
    own.wait()

    @pl.loop(1, n)
    def _(d):
        spread_arrival(d).wait_recv()

    for t in range(n):
        block = order[t]
        chosen[t] = spread[old_ref[block // 2], lax.rem(block, 2)]

    @pl.loop(1, n)
    def _(d):
        gather_copy(d).start()

    keep = pltpu.make_async_copy(chosen.at[me], got.at[me], own_sem.at[1])
    keep.start()
    for c in range(chunks):
        cols = pl.ds(c * cw, cw)
        gin[cols, :] = jnp.dot(p_t, x_buf[:, cols], preferred_element_type=jnp.float32).T
    tiles = width // 128
    lines = block_rows // tiles
    for b in range(chips):
        start = b * block_rows * 2
        low = gin[pl.ds(start, block_rows, stride=2), :]
        high = gin[pl.ds(start + 1, block_rows, stride=2), :]
        blocks[b] = jnp.concatenate([low, high], axis=1).astype(jnp.bfloat16)
    for b in range(chips):
        for t in range(tiles):
            turn[pl.ds(t, lines, stride=tiles), :] = gout[b * lines : (b + 1) * lines, t * 128 : (t + 1) * 128]
        blocks[chips + b] = turn[...].astype(jnp.bfloat16)

    pairs = chips // 2
    lane = lax.rem(chip, 2)
    pair = chip // 2

    def near_copy(to):
        return pltpu.make_async_remote_copy(
            outbox.at[to], near.at[to], s1.at[to], r1.at[to], device_id={"dp": sibling}, device_id_type=MESH
        )

    def mid_copy(at):
        return pltpu.make_async_remote_copy(
            summed.at[at * 2 + 1 - lane], mid.at[at], s3.at[at], r3.at[at],
            device_id={"dp": (pair * 2 + 1 - lane) * 2 + core}, device_id_type=MESH,
        )

    def far_copy(d):
        to = lax.rem(pair + d, pairs) * 2 + lane
        return pltpu.make_async_remote_copy(
            summed.at[to], far.at[d], s2.at[d], r2.at[d],
            device_id={"dp": to * 2 + core}, device_id_type=MESH,
        )

    for side in (1 - lane, lane):

        @pl.loop(1, pairs + 1)
        def _(step):
            to = lax.rem(pair + step, pairs) * 2 + side
            outbox[to] = blocks[order[to * 2 + 1 - core]]
            near_copy(to).start()

    @pl.loop(1, pairs + 1)
    def _(step):
        at = lax.rem(pair + step, pairs)
        to = at * 2 + 1 - lane
        near_copy(to).wait_recv()
        summed[to] = (
            blocks[order[to * 2 + core]].astype(jnp.float32) + near[to].astype(jnp.float32)
        ).astype(jnp.bfloat16)
        mid_copy(at).start()

    @pl.loop(1, pairs)
    def _(d):
        at = lax.rem(pair + d, pairs)
        to = at * 2 + lane
        near_copy(to).wait_recv()
        mid_copy(at).wait_recv()
        summed[to] = (
            blocks[order[to * 2 + core]].astype(jnp.float32)
            + near[to].astype(jnp.float32)
            + mid[at].astype(jnp.float32)
        ).astype(jnp.bfloat16)
        far_copy(d).start()

    near_copy(chip).wait_recv()
    mid_copy(pair).wait_recv()
    total_ref[...] = (
        blocks[order[me]].astype(jnp.float32) + near[chip].astype(jnp.float32) + mid[pair].astype(jnp.float32)
    )
    keep.wait()

    @pl.loop(1, n)
    def _(d):
        gather_arrival(d).wait_recv()

    for t in range(n):
        place = pl.ds(t * part, part)
        held = got[t].astype(jnp.float32)
        first_ref[place, :] = held[:part, :]
        second_ref[place, :] = held[slab : slab + part, :]

    @pl.loop(1, pairs)
    def _(d):
        far_copy(d).wait_recv()
        total_ref[...] += far[d].astype(jnp.float32)

    w_copy.wait_send()
    p_copy.wait_send()
    forward.wait_send()

    @pl.loop(1, n)
    def _(d):
        spread_copy(d).wait_send()
        gather_copy(d).wait_send()

    @pl.loop(0, chips)
    def _(d):
        near_copy(d).wait_send()

    @pl.loop(0, pairs)
    def _(d):
        mid_copy(d).wait_send()

    @pl.loop(1, pairs)
    def _(d):
        far_copy(d).wait_send()


def relay(n, new_owner, old_owner, x, loss, win, wout, first, second):
    rows, width = x.shape
    rank = win.shape[0]
    chunks = width // column_width(width)
    block_rows = first.shape[0] // 2
    slab = -(-(block_rows // n) // 8) * 8
    dma = pltpu.SemaphoreType.DMA
    bf16, f32 = jnp.bfloat16, jnp.float32
    group = pltpu.VMEM((n // 2, block_rows, 128), bf16)
    fewer = pltpu.VMEM((n // 4, block_rows, 128), bf16)
    lines = jax.ShapeDtypeStruct((block_rows, 128), f32)
    return pl.pallas_call(
        functools.partial(relay_kernel, n, block_rows),
        out_shape=(
            jax.ShapeDtypeStruct((rows, rank), bf16),
            jax.ShapeDtypeStruct((rank, width), bf16),
            jax.ShapeDtypeStruct((rows, rank), bf16),
            lines, lines, lines,
        ),
        in_specs=[SMEM, SMEM, ANY, ANY, VMEM, VMEM, VMEM, VMEM],
        out_specs=(VMEM,) * 6,
        scratch_shapes=[
            pltpu.SMEM((n,), jnp.int32),
            pltpu.VMEM(x.shape, bf16),
            pltpu.VMEM(x.shape, bf16),
            pltpu.VMEM((rows, rank), bf16),
            pltpu.VMEM((n, 2, 2 * slab, 128), bf16),
            pltpu.VMEM((n, 2, 2 * slab, 128), bf16),
            pltpu.VMEM((n, 2 * slab, 128), bf16),
            pltpu.VMEM((n, 2 * slab, 128), bf16),
            pltpu.VMEM((width, rank), f32),
            pltpu.VMEM((rank, width), f32),
            pltpu.VMEM((block_rows, 128), f32),
            pltpu.VMEM((n, block_rows, 128), bf16),
            group, group, group, fewer, fewer,
            dma((chunks,)), dma((chunks,)), dma, dma, dma, dma, dma, dma,
            dma((n,)), dma((n,)), dma((n,)), dma((n,)), dma((2,)),
            dma((n // 2,)), dma((n // 2,)), dma((n // 4,)), dma((n // 4,)), dma((n // 4,)), dma((n // 4,)),
        ],
        compiler_params=pltpu.CompilerParams(collective_id=0, has_side_effects=True),
        name="relay",
    )(new_owner, old_owner, x, loss, win, wout, first, second)


def emit_kernel(
    plan_ref, l_hbm, p_up_ref, w_up_ref, p_ref, win_ref, total_ref, m_ref, v_ref,
    out_hbm, u_ref, first_ref, second_ref,
    l_buf, o_buf, l_sem, o_sem,
):
    rank, width = win_ref.shape
    micro_count, tok_rows, _ = out_hbm.shape
    cw = column_width(width)
    chunks = width // cw
    loads = []
    for c in range(chunks):
        cols = pl.ds(c * cw, cw)
        loads.append(pltpu.make_async_copy(l_hbm.at[:, cols], l_buf.at[:, cols], l_sem.at[c]))
        loads[-1].start()
    adam(total_ref[...], m_ref[...], v_ref[...], u_ref, first_ref, second_ref)
    is_relayed = lax.axis_index("section") == 0
    p_up = jnp.where(is_relayed, p_up_ref[...].astype(jnp.float32), 0.0).astype(jnp.bfloat16)
    p_now = p_ref[...]
    stores = []
    for c in range(chunks):
        cols = pl.ds(c * cw, cw)
        loads[c].wait()
        incoming = (
            l_buf[:, cols].astype(jnp.float32)
            + jnp.dot(p_up, w_up_ref[:, cols], preferred_element_type=jnp.float32)
        ).astype(jnp.bfloat16)
        o_buf[:, cols] = (
            incoming.astype(jnp.float32) + jnp.dot(p_now, win_ref[:, cols], preferred_element_type=jnp.float32)
        ).astype(jnp.bfloat16)
        for m in range(micro_count):
            store = pltpu.make_async_copy(
                o_buf.at[pl.ds(pl.multiple_of(plan_ref[m] * tok_rows, tok_rows), tok_rows), cols],
                out_hbm.at[m, :, cols],
                o_sem.at[c, m],
            )
            store.start()
            stores.append(store)
    for store in stores:
        store.wait()


def emit(micro_count, plan, loss, p_up, w_up, p_now, win, total, m, v):
    rows, width = loss.shape
    chunks = width // column_width(width)
    dma = pltpu.SemaphoreType.DMA
    lines = jax.ShapeDtypeStruct(m.shape, jnp.float32)
    return pl.pallas_call(
        emit_kernel,
        out_shape=(
            jax.ShapeDtypeStruct((micro_count, rows // micro_count, width), jnp.bfloat16),
            lines, lines, lines,
        ),
        in_specs=[SMEM, ANY] + [VMEM] * 7,
        out_specs=(ANY, VMEM, VMEM, VMEM),
        scratch_shapes=[
            pltpu.VMEM(loss.shape, jnp.bfloat16),
            pltpu.VMEM(loss.shape, jnp.bfloat16),
            dma((chunks,)), dma((chunks, micro_count)),
        ],
        name="emit",
    )(plan, loss, p_up, w_up, p_now, win, total, m, v)


def adam(total, m, v, u_ref, first_ref, second_ref):
    grads = total / loss_scale
    first_next = beta_one * m + (1.0 - beta_one) * grads
    second_next = beta_two * v + (1.0 - beta_two) * grads * grads
    first_ref[...] = first_next
    second_ref[...] = second_next
    u_ref[...] = (
        first_next
        / (1.0 - beta_one**adam_step)
        / (jnp.sqrt(second_next / (1.0 - beta_two**adam_step)) + adam_eps)
    )


def reduce_kernel(
    n, q_ref, m_ref, v_ref, u_ref, first_ref, second_ref,
    near, summed, far, s1, r1, s2, r2,
):
    me = lax.axis_index("dp")
    core = lax.rem(me, 2)
    chip = me // 2
    chips = n // 2
    sibling = me + 1 - 2 * core
    greet(n, me, None)

    def near_copy(d):
        to = lax.rem(chip + d, chips)
        return pltpu.make_async_remote_copy(
            q_ref.at[(1 - core) * chips + to], near.at[to], s1.at[d], r1.at[d],
            device_id={"dp": sibling}, device_id_type=MESH,
        )

    def far_copy(d):
        to = lax.rem(chip + d, chips)
        return pltpu.make_async_remote_copy(
            summed.at[to], far.at[d], s2.at[d], r2.at[d],
            device_id={"dp": to * 2 + core}, device_id_type=MESH,
        )

    @pl.loop(1, chips + 1)
    def _(step):
        near_copy(lax.rem(step, chips)).start()

    @pl.loop(1, chips)
    def _(d):
        to = lax.rem(chip + d, chips)
        near_copy(d).wait_recv()
        summed[to] = (
            q_ref[core * chips + to].astype(jnp.float32) + near[to].astype(jnp.float32)
        ).astype(jnp.bfloat16)
        far_copy(d).start()

    near_copy(0).wait_recv()
    total = q_ref[core * chips + chip].astype(jnp.float32) + near[chip].astype(jnp.float32)
    first_ref[...] = total

    @pl.loop(1, chips)
    def _(d):
        far_copy(d).wait_recv()
        first_ref[...] += far[d].astype(jnp.float32)

    adam(first_ref[...], m_ref[...], v_ref[...], u_ref, first_ref, second_ref)

    @pl.loop(0, chips)
    def _(d):
        near_copy(d).wait_send()

    @pl.loop(1, chips)
    def _(d):
        far_copy(d).wait_send()


def reduce_adam(n, blocks, m, v):
    lines = m.shape
    dma = pltpu.SemaphoreType.DMA
    shape = jax.ShapeDtypeStruct(lines, jnp.float32)
    group = pltpu.VMEM((n // 2,) + lines, jnp.bfloat16)
    return pl.pallas_call(
        functools.partial(reduce_kernel, n),
        out_shape=(shape,) * 3,
        in_specs=[VMEM] * 3,
        out_specs=(VMEM,) * 3,
        scratch_shapes=[group, group, group] + [dma((n // 2,))] * 4,
        compiler_params=pltpu.CompilerParams(collective_id=1, has_side_effects=True),
        name="reduce_adam",
    )(blocks, m, v)


def passed_along(value, axis, steps):
    count = lax.axis_size(axis)
    first, last = (max(0, -steps), min(count, count - steps))
    return lax.ppermute(value, axis, [(source, source + steps) for source in range(first, last)])


def silu_slope(pre_value):
    gate_value = jax.nn.sigmoid(pre_value)
    return gate_value * (1.0 + pre_value * (1.0 - gate_value))


def per_device(
    activations,
    loss_grads,
    adapter_in,
    adapter_out,
    first_moment,
    second_moment,
    old_owner,
    new_owner,
    plan,
):
    sections = lax.axis_size("section")
    section_index = lax.axis_index("section")
    replicas = lax.axis_size("dp")
    my_index = lax.axis_index("dp")
    weight_in = adapter_in[0]
    weight_out = adapter_out[0]
    inputs_all = activations[0]
    micro_count = inputs_all.shape[0]
    tok_rows = inputs_all.shape[1]
    width = inputs_all.shape[2]
    owners_old = old_owner[0]
    owners_new = new_owner[0]
    block_len = first_moment.shape[2] // 2
    replica_ids = jnp.arange(replicas, dtype=jnp.int32)
    new_block = jnp.sum(jnp.where(owners_new == my_index, replica_ids, 0))

    def drain_turn(turn_index, state):
        previous, grad_in, grad_out, emitted = state
        received = passed_along(previous, "section", -1)
        slot = turn_index - (sections - 1 - section_index)
        is_valid = (slot >= 0) & (slot < micro_count)
        clamped = jnp.clip(slot, 0, micro_count - 1)
        micro = lax.dynamic_index_in_dim(plan, clamped, 0, keepdims=False)
        section_input = lax.dynamic_index_in_dim(inputs_all, micro, 0, keepdims=False)
        from_loss = lax.dynamic_index_in_dim(loss_grads, micro, 0, keepdims=False)
        incoming = jnp.where(section_index == sections - 1, from_loss, received)
        pre_value = jnp.dot(section_input, weight_in, preferred_element_type=jnp.float32)
        hidden = jax.nn.silu(pre_value).astype(jnp.bfloat16)
        act_grad = jnp.dot(incoming, weight_out.T, preferred_element_type=jnp.float32)
        pre_grad = (act_grad * silu_slope(pre_value)).astype(jnp.bfloat16)
        input_grad = (
            incoming.astype(jnp.float32)
            + jnp.dot(pre_grad, weight_in.T, preferred_element_type=jnp.float32)
        ).astype(jnp.bfloat16)
        valid_weight = is_valid.astype(jnp.float32)
        grad_in = grad_in + valid_weight * jnp.dot(
            section_input.T, pre_grad, preferred_element_type=jnp.float32
        )
        grad_out = grad_out + valid_weight * jnp.dot(
            hidden.T, incoming, preferred_element_type=jnp.float32
        )
        earlier = lax.dynamic_index_in_dim(emitted, clamped, 0, keepdims=False)
        written = jnp.where(is_valid, input_grad, earlier)
        emitted = lax.dynamic_update_index_in_dim(emitted, written, clamped, 0)
        return (input_grad, grad_in, grad_out, emitted)

    start_state = (
        jnp.zeros((tok_rows, width), jnp.bfloat16),
        jnp.zeros(weight_in.shape, jnp.float32),
        jnp.zeros(weight_out.shape, jnp.float32),
        jnp.zeros((micro_count, tok_rows, width), jnp.bfloat16),
    )
    place_of_block = owners_new % 2 * (replicas // 2) + owners_new // 2
    lines = (block_len // 128, 128)
    if sections == 2 and replicas % 4 == 0 and block_len % (128 * replicas) == 0:
        rows = micro_count * tok_rows
        flat_inputs = inputs_all.reshape(rows, width)
        flat_loss = loss_grads.reshape(rows, width)
        turned_in = weight_in.T
        row_lines = (2 * block_len // 128, 128)
        p_up, w_up, p_now, total, first_old, second_old = relay(
            replicas, owners_new, owners_old, flat_inputs, flat_loss, turned_in, weight_out,
            first_moment.reshape(row_lines), second_moment.reshape(row_lines),
        )
        emitted, update, first_next, second_next = emit(
            micro_count, plan, flat_loss, p_up, w_up, p_now, turned_in, total, first_old, second_old
        )
        shape = (1, 1, block_len)
        return (emitted[None], update.reshape(shape), first_next.reshape(shape), second_next.reshape(shape))
    last_grad, grad_in, grad_out, emitted = lax.fori_loop(
        0, micro_count + sections - 1, drain_turn, start_state
    )
    partial_value = jnp.concatenate([grad_in.reshape(-1), grad_out.reshape(-1)])
    block_at = jnp.sum(
        jnp.where(place_of_block[None, :] == replica_ids[:, None], replica_ids[None, :], 0), axis=1
    )
    blocks = jnp.take(partial_value.astype(jnp.bfloat16).reshape((replicas,) + lines), block_at, axis=0)
    old_count = owners_old.shape[0]
    piece_len = 2 * block_len // replicas
    first_pieces = first_moment[0, 0].reshape(replicas, piece_len)
    second_pieces = second_moment[0, 0].reshape(replicas, piece_len)
    first_spread = lax.all_to_all(first_pieces, "dp", split_axis=0, concat_axis=0, tiled=True)
    second_spread = lax.all_to_all(second_pieces, "dp", split_axis=0, concat_axis=0, tiled=True)
    first_held = jnp.take(first_spread, owners_old, axis=0)
    second_held = jnp.take(second_spread, owners_old, axis=0)
    my_half = my_index // old_count
    targets = owners_new.reshape(-1, 2)
    target_of_block = jnp.where(my_half == 0, targets[:, 0], targets[:, 1])
    picker = (target_of_block[None, :] == replica_ids[:, None]).astype(jnp.float32)
    first_out = jnp.dot(picker, first_held, precision=lax.Precision.HIGHEST)
    second_out = jnp.dot(picker, second_held, precision=lax.Precision.HIGHEST)
    first_got = lax.all_to_all(first_out, "dp", split_axis=0, concat_axis=0, tiled=True)
    second_got = lax.all_to_all(second_out, "dp", split_axis=0, concat_axis=0, tiled=True)
    half_start = new_block % 2 * old_count
    first_mine = lax.dynamic_slice_in_dim(first_got, half_start, old_count, 0).reshape(-1)
    second_mine = lax.dynamic_slice_in_dim(second_got, half_start, old_count, 0).reshape(-1)
    update, first_next, second_next = reduce_adam(
        replicas, blocks, first_mine.reshape(lines), second_mine.reshape(lines)
    )
    shape = (1, 1, block_len)
    return (emitted[None], update.reshape(shape), first_next.reshape(shape), second_next.reshape(shape))


def solution(mesh):
    placed = (
        P("section", None, "dp", None),
        P(None, "dp", None),
        P("section", None, None),
        P("section", None, None),
        P("section", "dp", None),
        P("section", "dp", None),
        P("section", None),
        P("section", None),
        P(),
    )
    return jax.shard_map(
        per_device,
        mesh=mesh,
        in_specs=placed,
        out_specs=(
            P("section", None, "dp", None),
            P("section", "dp", None),
            P("section", "dp", None),
            P("section", "dp", None),
        ),
        check_vma=False,
    )
```
